32 devices in a mesh: tm: 32 (over z, y, x, core), asset: 1.
Axes of the slice: x: 2, y: 2, z: 4, core: 2. Of those that a mesh axis runs over, the one named last changes fastest.
Arguments:
- returns: float32 [512, 2048], P('tm', 'asset'), may hold values from -6 to 6
- windows: int32 [32], P('tm'), may hold values from 20 to 250, as said below
- listed_from: int32 [2048], replicated, may hold values from 0 to 255
- listed_until: int32 [2048], replicated, may hold values from 256 to 512
Outputs:
- correlation: float32 [32, 2048, 2048], P('tm', None, 'asset')
The draws below stay inside these ranges and needn't reach their ends.
Inputs may be any that keep to these rules, and one draw needn't show every extreme that they name: `windows`: each window length is one of the four horizons max(256 * h // 256, 2) for h in 20, 60, 120, 250; the shortest and the longest both occur in every draw.
All inputs are finite; a program needn't handle non-finite values.
Results may differ from the reference program's by a relative error of at most 0.0003.
Values sent between devices are 32-bit elements; how exact they have to be, the bound alone decides.
No kernel may reach another device: no remote copies, remote signals or barrier semaphores. Data moves between devices by JAX's collectives and lax.ppermute only.
A program may use at most 128 MiB of HBM per device.

```python
import jax
import jax.numpy as jnp
from jax import lax

ASSETS = 2048
SPAN = 256
GROUP = 16
DAYS = 512
N_TM = 32


def draw_windows(key, part):
    horizons = jnp.array([20, 60, 120, 250], jnp.int32)
    key_pick = jax.random.fold_in(key, 11)
    key_spot = jax.random.fold_in(key, 23)
    chosen_idx = jax.random.randint(key_pick, (N_TM,), 0, 4)
    special = jax.random.randint(key_spot, (), 0, N_TM)
    position = jnp.arange(N_TM, dtype=jnp.int32)
    chosen_idx = jnp.where(position == special, 3, chosen_idx)
    chosen_idx = jnp.where(position == (special + 1) % N_TM, 0, chosen_idx)
    lengths = jnp.sum(jnp.where(chosen_idx[:, None] == jnp.arange(4, dtype=jnp.int32)[None, :], horizons[None, :], 0), axis=1)
    return jnp.maximum(SPAN * lengths // 256, 2).astype(jnp.int32)


def set_ends(values, own_key, low, high):
    index_at = [jax.random.randint(jax.random.fold_in(own_key, axis), (), 0, length) for axis, length in enumerate(values.shape)]
    main_axis = values.shape.index(max(values.shape))
    neighbour = index_at[:main_axis] + [(index_at[main_axis] + 1) % values.shape[main_axis]] + index_at[main_axis + 1:]
    return values.at[tuple(index_at)].set(low).at[tuple(neighbour)].set(high)


def shard_levels(own_key, extent, cuts, low, largest):
    factor_of, own = 1.0, jax.random.fold_in(own_key, 6)
    for dim, shards_of in cuts:
        steps = jnp.exp(jax.random.uniform(jax.random.fold_in(own, dim), (shards_of,), jnp.float32, low / len(cuts), largest / len(cuts)))
        factor_of = factor_of * jnp.repeat(steps, extent[dim] // shards_of).reshape([-1 if axis == dim else 1 for axis in range(len(extent))])
    return factor_of


def gaussian(own_key, shape, deviation, most, shards=(), kind=jnp.bfloat16):
    values = deviation * jax.random.normal(own_key, shape, jnp.float32)
    if shards:
        values = values * shard_levels(own_key, shape, shards, -0.22, 0.18)
    return jnp.clip(values, -most, most).astype(kind)


def setup_inputs(seed: int = 0) -> dict:
    key_of = jax.random.split(jax.random.key(seed), 5)
    return {
        "returns": gaussian(key_of[0], (DAYS, ASSETS), 1.0, 6.0, ((0, 32),), jnp.float32),
        "windows": draw_windows(jax.random.fold_in(key_of[4], 71), 0),
        "listed_from": set_ends(jax.random.randint(key_of[2], (ASSETS,), 0, DAYS // 2), jax.random.fold_in(key_of[2], 1), 0, (DAYS // 2) - 1).astype(jnp.int32),
        "listed_until": set_ends(jax.random.randint(key_of[3], (ASSETS,), DAYS // 2, DAYS + 1), jax.random.fold_in(key_of[3], 1), DAYS // 2, DAYS).astype(jnp.int32),
    }


highest = lax.Precision.HIGHEST

def cross_days(left_side, right_side):
    return lax.dot_general(left_side, right_side, (((0,), (0,)), ((), ())), precision=highest, preferred_element_type=jnp.float32)

def correlate(cross_terms, sum_left, sum_right, square_left, square_right, pair_count):
    pairs = jnp.maximum(pair_count, 1.0)
    covariance = cross_terms - sum_left * sum_right / pairs
    var_left = jnp.maximum(square_left - sum_left * sum_left / pairs, 1.0)
    var_right = jnp.maximum(square_right - sum_right * sum_right / pairs, 1.0)
    return covariance / jnp.sqrt(var_left * var_right)

def reference(returns, windows, listed_from, listed_until):
    padded = jnp.concatenate([jnp.zeros((SPAN - GROUP, ASSETS), jnp.float32), returns], axis=0)

    def evaluate(evaluation):
        end_day = (evaluation + 1) * GROUP - 1
        window_rows = lax.dynamic_slice_in_dim(padded, (evaluation * GROUP).astype(jnp.int32), SPAN, 0)
        day_index = end_day - SPAN + 1 + jnp.arange(SPAN, dtype=jnp.int32)
        inside = (day_index > end_day - windows[evaluation]) & (day_index >= 0)
        alive = inside[:, None] & (listed_from[None, :] <= day_index[:, None]) & (day_index[:, None] < listed_until[None, :])
        listed = alive.astype(jnp.float32)
        values = window_rows * listed
        squared = values * values
        cross_terms = cross_days(values, values)
        sum_terms = cross_days(values, listed)
        square_terms = cross_days(squared, listed)
        pair_count = cross_days(listed, listed)
        return correlate(cross_terms, sum_terms, sum_terms.T, square_terms, square_terms.T, pair_count)
    return lax.map(evaluate, jnp.arange(N_TM, dtype=jnp.int32))
```

```python
import functools

import jax
import jax.numpy as jnp
import numpy as np
from jax import lax
from jax.experimental import pallas as pl
from jax.experimental.pallas import tpu as pltpu
from jax.sharding import PartitionSpec as P

SPAN = 256
TILE = 256
UNROLL = 4


def cycle(array, axis, by):
    devices = lax.axis_size(axis)
    return lax.ppermute(array, axis, [(i, (i + by) % devices) for i in range(devices)])


def swap(array, axis, by):
    devices = lax.axis_size(axis)
    return lax.ppermute(array, axis, [(i, i ^ by) for i in range(devices)])


def gather_span(rows, axis, members):
    height = rows.shape[0]
    member = lax.rem(lax.axis_index(axis), members)
    before = cycle(rows, axis, members)
    before2 = cycle(before, axis, members)
    stack = jnp.concatenate([before2, before, rows], axis=0)

    def for_other(by):
        start = jnp.where((member ^ by) > member, height, 0)
        return lax.dynamic_slice_in_dim(stack, start, 2 * height, 0)

    got = [swap(for_other(by), axis, by) for by in range(2, members, 2)]
    relay = jnp.concatenate([for_other(1), *got], axis=0)
    relayed = swap(relay, axis, 1)
    return [before, rows, *got, relayed]


def block_days(axis, members, height):
    position = lax.axis_index(axis)
    member = lax.rem(position, members)
    group = position // members
    order = [0] + list(range(2, members, 2)) + [1] + [by ^ 1 for by in range(2, members, 2)]
    other = member ^ jnp.array(order, jnp.int32)
    newest = jnp.where(other > member, group - 1, group)
    blocks = jnp.stack([(newest - 1) * members + other, newest * members + other], axis=1).reshape(-1)
    return (blocks * height).astype(jnp.int32)


def correlation_kernel(sizes, *refs):
    heights, height, mirrored, plain, first_tile = sizes
    pieces = refs[: len(heights)]
    (starts, bounds, tiles_m, tiles_p, born, gone, out) = refs[len(heights) : len(heights) + 7]
    (hi_r, lo_r, sq_r, sl_r, live_r, hi_l, lo_l, sq_l, sl_l, live_l, sums, buf_m, buf_t, buf_p, sem_m, sem_t, sem_p) = refs[
        len(heights) + 7 :
    ]
    assets = born.shape[1]
    f32, bf16 = jnp.float32, jnp.bfloat16

    def split(x):
        high = x.astype(bf16)
        return high, (x - high.astype(f32)).astype(bf16)

    def prepare(step, carry):
        at = pl.multiple_of(step * TILE, TILE)
        cols = pl.ds(at, TILE)
        low = jnp.maximum(born[:, cols], bounds[0])
        high = jnp.minimum(gone[:, cols], bounds[1])
        values, lives = [], []
        block = 0
        for piece, rows in zip(pieces, heights):
            for row in range(0, rows, height):
                day = starts[block] + lax.broadcasted_iota(jnp.int32, (height, TILE), 0)
                block += 1
                live = jnp.where((day >= low) & (day < high), 1.0, 0.0).astype(f32)
                lives.append(live)
                values.append(piece[pl.ds(row, height), cols] * live)
        value = jnp.concatenate(values, axis=0)
        live = jnp.concatenate(lives, axis=0)
        hi_r[:, cols], lo_r[:, cols] = split(value)
        sq_r[:, cols], sl_r[:, cols] = split(value * value)
        live_r[:, cols] = live.astype(bf16)
        value = value.T
        hi_l[cols, :], lo_l[cols, :] = split(value)
        sq_l[cols, :], sl_l[cols, :] = split(value * value)
        live_l[cols, :] = live.T.astype(bf16)
        return carry

    lax.fori_loop(0, assets // TILE, prepare, 0)

    def body(*accs):
        first, second = accs[:4], accs[4:]

        def clear():
            for acc in accs:
                sums[0, 0] = pltpu.matmul_pop(acc)

        clear()

        def products(i, j, turn):
            rows = pl.ds(pl.multiple_of(i * TILE, TILE), TILE)
            cols = pl.ds(pl.multiple_of(j * TILE, TILE), TILE)
            f = [first[(turn * 3 + k) % 4] for k in range(3)]
            s = [second[(turn * 3 + k) % 4] for k in range(3)]
            push, acc = pltpu.matmul_push_rhs, pltpu.matmul_acc_lhs
            push(live_r[:, cols], staging_register=0, mxu_index=0)
            push(hi_r[:, cols], staging_register=0, mxu_index=1)
            acc(f[0], live_l[rows, :], load_staged_rhs=0)
            acc(s[0], live_l[rows, :], load_staged_rhs=0)
            push(hi_r[:, cols], staging_register=1, mxu_index=0)
            push(lo_r[:, cols], staging_register=1, mxu_index=1)
            acc(f[1], hi_l[rows, :])
            acc(s[0], live_l[rows, :], load_staged_rhs=1)
            push(sq_r[:, cols], staging_register=0, mxu_index=1)
            acc(f[1], lo_l[rows, :])
            acc(s[1], live_l[rows, :], load_staged_rhs=0)
            push(sl_r[:, cols], staging_register=1, mxu_index=1)
            acc(f[2], hi_l[rows, :], load_staged_rhs=1)
            push(lo_r[:, cols], staging_register=0, mxu_index=0)
            acc(s[1], live_l[rows, :], load_staged_rhs=1)
            push(live_r[:, cols], staging_register=0, mxu_index=1)
            acc(f[2], lo_l[rows, :])
            acc(s[2], sq_l[rows, :], load_staged_rhs=0)
            acc(f[2], hi_l[rows, :], load_staged_rhs=0)
            acc(s[2], sl_l[rows, :])
            where = turn % 2
            for k in range(3):
                sums[where, 2 * k] = pltpu.matmul_pop(f[k])
                sums[where, 2 * k + 1] = pltpu.matmul_pop(s[k])

        def combine(turn, target, mirror):
            where = turn % 2
            step = 16
            for row in range(0, TILE, step):
                rows = pl.ds(row, step)
                pairs = jnp.maximum(sums[where, 0, rows, :], 1.0)
                right = sums[where, 1, rows, :]
                left = sums[where, 2, rows, :]
                var_right = jnp.maximum(pairs * sums[where, 3, rows, :] - right * right, pairs)
                var_left = jnp.maximum(pairs * sums[where, 5, rows, :] - left * left, pairs)
                covariance = pairs * sums[where, 4, rows, :] - left * right
                target[rows, :] = covariance * lax.rsqrt(var_left * var_right)
            if mirror is not None:
                mirror[...] = target[...].T

        def tiles(table, step, turns):
            return [(table[0, step * turns + u], table[1, step * turns + u]) for u in range(turns)]

        def place(i, j):
            rows = pl.ds(pl.multiple_of(i * TILE, TILE), TILE)
            cols = pl.ds(pl.multiple_of((j - first_tile_of()) * TILE, TILE), TILE)
            return out.at[rows, cols]

        def first_tile_of():
            return bounds[2] if first_tile else 0

        def copies(table, step, turns, buf, sem, flip):
            slot = lax.rem(step, 2)
            for u, (i, j) in enumerate(tiles(table, step, turns)):
                spot = place(j, i) if flip else place(i, j)
                yield pltpu.make_async_copy(buf.at[slot, u], spot, sem.at[slot, u])

        def run(table, steps, turns, buf, sem, mirror_buf, mirror_sem):
            def waits(step):
                for copy in copies(table, step, turns, buf, sem, False):
                    copy.wait()
                if mirror_buf is not None:
                    for copy in copies(table, step, turns, mirror_buf, mirror_sem, True):
                        copy.wait()

            def one(step, carry):
                slot = lax.rem(step, 2)

                @pl.when(step >= 2)
                def _():
                    waits(step - 2)

                where = tiles(table, step, turns)
                for u in range(turns):
                    products(*where[u], u)
                    if u:
                        combine(u - 1, buf.at[slot, u - 1], None if mirror_buf is None else mirror_buf.at[slot, u - 1])
                combine(turns - 1, buf.at[slot, turns - 1], None if mirror_buf is None else mirror_buf.at[slot, turns - 1])
                for copy in copies(table, step, turns, buf, sem, False):
                    copy.start()
                if mirror_buf is not None:
                    for copy in copies(table, step, turns, mirror_buf, mirror_sem, True):
                        copy.start()
                return carry

            lax.fori_loop(0, steps, one, 0)
            return lambda: [waits(step) for step in range(max(steps - 2, 0), steps)]

        ends = []
        if mirrored[0]:
            ends.append(run(tiles_m, *mirrored, buf_m, sem_m, buf_t, sem_t))
        ends.append(run(tiles_p, *plain, buf_p, sem_p, None, None))
        for end in ends:
            end()

    pl.run_scoped(body, *([pltpu.ACC(0)((TILE, TILE), f32)] * 4 + [pltpu.ACC(1)((TILE, TILE), f32)] * 4))


def turns_of(count):
    return max(t for t in range(1, UNROLL + 1) if count % t == 0)


def correlation(pieces, starts, bounds, born, gone, height, width, whole):
    assets = born.shape[0]
    every = assets // TILE
    own = width // TILE
    if whole:
        mirrored = [(i, j) for j in range(every) for i in range(j)]
        plain = [(i, i) for i in range(every)]
        first = jnp.int32(0)
    else:
        mirrored = []
        plain = [(i, j) for j in range(own) for i in range(every)]
        first = (lax.axis_index("asset") * own).astype(jnp.int32)
    table_m = jnp.array(np.array(mirrored or [(0, 0)], np.int32).T)
    table_p = jnp.array(np.array(plain, np.int32).T)
    if not whole:
        table_p = table_p + jnp.stack([jnp.int32(0), first])[:, None]
    bounds = jnp.concatenate([bounds, first[None]])
    turns_m = turns_of(len(mirrored)) if mirrored else 1
    turns_p = turns_of(len(plain))
    sizes = (
        tuple(p.shape[0] for p in pieces),
        height,
        (len(mirrored) // turns_m, turns_m),
        (len(plain) // turns_p, turns_p),
        not whole,
    )
    f32, bf16 = jnp.float32, jnp.bfloat16
    vmem = pl.BlockSpec(memory_space=pltpu.VMEM)
    smem = pl.BlockSpec(memory_space=pltpu.SMEM)
    depth = SPAN
    flops = 12 * 2 * depth * TILE * TILE * (len(mirrored) + len(plain))
    return pl.pallas_call(
        functools.partial(correlation_kernel, sizes),
        out_shape=jax.ShapeDtypeStruct((assets, width), f32),
        in_specs=[vmem] * len(pieces) + [smem] * 4 + [vmem] * 2,
        out_specs=pl.BlockSpec(memory_space=pl.ANY),
        scratch_shapes=[pltpu.VMEM((depth, assets), bf16)] * 5
        + [pltpu.VMEM((assets, depth), bf16)] * 5
        + [
            pltpu.VMEM((2, 6, TILE, TILE), f32),
            pltpu.VMEM((2, turns_m, TILE, TILE), f32),
            pltpu.VMEM((2, turns_m, TILE, TILE), f32),
            pltpu.VMEM((2, turns_p, TILE, TILE), f32),
            pltpu.SemaphoreType.DMA((2, turns_m)),
            pltpu.SemaphoreType.DMA((2, turns_m)),
            pltpu.SemaphoreType.DMA((2, turns_p)),
        ],
        cost_estimate=pl.CostEstimate(flops=flops, bytes_accessed=4 * assets * width, transcendentals=assets * width),
        compiler_params=pltpu.CompilerParams(vmem_limit_bytes=56 * 2**20),
    )(*pieces, starts, bounds, table_m, table_p, born[None], gone[None])


def on_device(returns, windows, listed_from, listed_until):
    height, width = returns.shape
    members = SPAN // height // 2
    rows = lax.all_gather(returns, "asset", axis=1, tiled=True)
    pieces = gather_span(rows, "tm", members)
    starts = block_days("tm", members, height)
    after = (lax.axis_index("tm") + 1) * height
    bounds = jnp.stack([jnp.maximum(after - windows[0], 0), after]).astype(jnp.int32)
    whole = lax.axis_size("asset") == 1
    return correlation(pieces, starts, bounds, listed_from, listed_until, height, width, whole)[None]


def solution(mesh):
    placed = (P("tm", "asset"), P("tm"), P(), P())
    step = jax.shard_map(on_device, mesh=mesh, in_specs=placed, out_specs=P("tm", None, "asset"), check_vma=False)

    def call(*args):
        with jax.sharding.use_abstract_mesh(mesh.abstract_mesh):
            return step(*args)

    return call
```

```python
import functools

import jax
import jax.numpy as jnp
import numpy as np
from jax import lax
from jax.experimental import pallas as pl
from jax.experimental.pallas import tpu as pltpu
from jax.sharding import PartitionSpec as P

SPAN = 256
TILE = 256
UNROLL = 4


def cycle(array, axis, by):
    devices = lax.axis_size(axis)
    return lax.ppermute(array, axis, [(i, (i + by) % devices) for i in range(devices)])


def swap(array, axis, by):
    devices = lax.axis_size(axis)
    return lax.ppermute(array, axis, [(i, i ^ by) for i in range(devices)])


def gather_span(rows, axis, members):
    member = lax.rem(lax.axis_index(axis), members)
    before = cycle(rows, axis, members)
    middle = [swap(before, axis, by) for by in range(2, members, 2)]
    before2 = cycle(before, axis, members)

    def outer(by):
        return jnp.where((member ^ by) > member, rows, before2)

    ends = [swap(outer(by), axis, by) for by in range(2, members, 2)]
    relayed = [swap(piece, axis, 1) for piece in (before, *middle, outer(1), *ends)]
    return [before, *middle, *relayed[: members // 2], rows, *ends, *relayed[members // 2 :]]


def block_days(axis, members, height):
    position = lax.axis_index(axis)
    member = lax.rem(position, members)
    group = position // members
    order = [0] + list(range(2, members, 2)) + [1] + [by ^ 1 for by in range(2, members, 2)]
    other = member ^ jnp.array(order, jnp.int32)
    middle = (group - 1) * members + other
    ends = jnp.where(other > member, group - 2, group) * members + other
    return (jnp.concatenate([middle, ends]) * height).astype(jnp.int32)


def correlation_kernel(sizes, *refs):
    heights, height, mirrored, plain, first_tile = sizes
    pieces = refs[: len(heights)]
    (starts, bounds, tiles_m, tiles_p, born, gone, out) = refs[len(heights) : len(heights) + 7]
    (hi_r, lo_r, sq_r, sl_r, live_r, hi_l, lo_l, sq_l, sl_l, live_l, sums, buf_m, buf_t, buf_p, sem_m, sem_t, sem_p) = refs[
        len(heights) + 7 :
    ]
    assets = born.shape[1]
    f32, bf16 = jnp.float32, jnp.bfloat16

    def split(x):
        high = x.astype(bf16)
        return high, (x - high.astype(f32)).astype(bf16)

    def prepare(step, carry):
        at = pl.multiple_of(step * TILE, TILE)
        cols = pl.ds(at, TILE)
        low = jnp.maximum(born[:, cols], bounds[0])
        high = jnp.minimum(gone[:, cols], bounds[1])
        values, lives = [], []
        block = 0
        for piece, rows in zip(pieces, heights):
            for row in range(0, rows, height):
                day = starts[block] + lax.broadcasted_iota(jnp.int32, (height, TILE), 0)
                block += 1
                live = jnp.where((day >= low) & (day < high), 1.0, 0.0).astype(f32)
                lives.append(live)
                values.append(piece[pl.ds(row, height), cols] * live)
        value = jnp.concatenate(values, axis=0)
        live = jnp.concatenate(lives, axis=0)
        hi_r[:, cols], lo_r[:, cols] = split(value)
        sq_r[:, cols], sl_r[:, cols] = split(value * value)
        live_r[:, cols] = live.astype(bf16)
        value = value.T
        hi_l[cols, :], lo_l[cols, :] = split(value)
        sq_l[cols, :], sl_l[cols, :] = split(value * value)
        live_l[cols, :] = live.T.astype(bf16)
        return carry

    lax.fori_loop(0, assets // TILE, prepare, 0)

    def body(*accs):
        first, second = accs[:4], accs[4:]

        def clear():
            for acc in accs:
                sums[0, 0] = pltpu.matmul_pop(acc)

        clear()

        def products(i, j, turn):
            rows = pl.ds(pl.multiple_of(i * TILE, TILE), TILE)
            cols = pl.ds(pl.multiple_of(j * TILE, TILE), TILE)
            f = [first[(turn * 3 + k) % 4] for k in range(3)]
            s = [second[(turn * 3 + k) % 4] for k in range(3)]
            push, acc = pltpu.matmul_push_rhs, pltpu.matmul_acc_lhs
            push(live_r[:, cols], staging_register=0, mxu_index=0)
            push(hi_r[:, cols], staging_register=0, mxu_index=1)
            acc(f[0], live_l[rows, :], load_staged_rhs=0)
            acc(s[0], live_l[rows, :], load_staged_rhs=0)
            push(hi_r[:, cols], staging_register=1, mxu_index=0)
            push(lo_r[:, cols], staging_register=1, mxu_index=1)
            acc(f[1], hi_l[rows, :])
            acc(s[0], live_l[rows, :], load_staged_rhs=1)
            push(sq_r[:, cols], staging_register=0, mxu_index=1)
            acc(f[1], lo_l[rows, :])
            acc(s[1], live_l[rows, :], load_staged_rhs=0)
            push(sl_r[:, cols], staging_register=1, mxu_index=1)
            acc(f[2], hi_l[rows, :], load_staged_rhs=1)
            push(lo_r[:, cols], staging_register=0, mxu_index=0)
            acc(s[1], live_l[rows, :], load_staged_rhs=1)
            push(live_r[:, cols], staging_register=0, mxu_index=1)
            acc(f[2], lo_l[rows, :])
            acc(s[2], sq_l[rows, :], load_staged_rhs=0)
            acc(f[2], hi_l[rows, :], load_staged_rhs=0)
            acc(s[2], sl_l[rows, :])
            where = turn % 2
            for k in range(3):
                sums[where, 2 * k] = pltpu.matmul_pop(f[k])
                sums[where, 2 * k + 1] = pltpu.matmul_pop(s[k])

        def combine(turn, target, mirror):
            where = turn % 2
            step = 16
            for row in range(0, TILE, step):
                rows = pl.ds(row, step)
                pairs = jnp.maximum(sums[where, 0, rows, :], 1.0)
                right = sums[where, 1, rows, :]
                left = sums[where, 2, rows, :]
                var_right = jnp.maximum(pairs * sums[where, 3, rows, :] - right * right, pairs)
                var_left = jnp.maximum(pairs * sums[where, 5, rows, :] - left * left, pairs)
                covariance = pairs * sums[where, 4, rows, :] - left * right
                target[rows, :] = covariance * lax.rsqrt(var_left * var_right)
            if mirror is not None:
                mirror[...] = target[...].T

        def tiles(table, step, turns):
            return [(table[0, step * turns + u], table[1, step * turns + u]) for u in range(turns)]

        def place(i, j):
            rows = pl.ds(pl.multiple_of(i * TILE, TILE), TILE)
            cols = pl.ds(pl.multiple_of((j - first_tile_of()) * TILE, TILE), TILE)
            return out.at[rows, cols]

        def first_tile_of():
            return bounds[2] if first_tile else 0

        def copies(table, step, turns, buf, sem, flip):
            slot = lax.rem(step, 2)
            for u, (i, j) in enumerate(tiles(table, step, turns)):
                spot = place(j, i) if flip else place(i, j)
                yield pltpu.make_async_copy(buf.at[slot, u], spot, sem.at[slot, u])

        def run(table, steps, turns, buf, sem, mirror_buf, mirror_sem):
            def waits(step):
                for copy in copies(table, step, turns, buf, sem, False):
                    copy.wait()
                if mirror_buf is not None:
                    for copy in copies(table, step, turns, mirror_buf, mirror_sem, True):
                        copy.wait()

            def one(step, carry):
                slot = lax.rem(step, 2)

                @pl.when(step >= 2)
                def _():
                    waits(step - 2)

                where = tiles(table, step, turns)
                for u in range(turns):
                    products(*where[u], u)
                    if u:
                        combine(u - 1, buf.at[slot, u - 1], None if mirror_buf is None else mirror_buf.at[slot, u - 1])
                combine(turns - 1, buf.at[slot, turns - 1], None if mirror_buf is None else mirror_buf.at[slot, turns - 1])
                for copy in copies(table, step, turns, buf, sem, False):
                    copy.start()
                if mirror_buf is not None:
                    for copy in copies(table, step, turns, mirror_buf, mirror_sem, True):
                        copy.start()
                return carry

            lax.fori_loop(0, steps, one, 0)
            return lambda: [waits(step) for step in range(max(steps - 2, 0), steps)]

        ends = []
        if mirrored[0]:
            ends.append(run(tiles_m, *mirrored, buf_m, sem_m, buf_t, sem_t))
        ends.append(run(tiles_p, *plain, buf_p, sem_p, None, None))
        for end in ends:
            end()

    pl.run_scoped(body, *([pltpu.ACC(0)((TILE, TILE), f32)] * 4 + [pltpu.ACC(1)((TILE, TILE), f32)] * 4))


def turns_of(count):
    return max(t for t in range(1, UNROLL + 1) if count % t == 0)


def correlation(pieces, starts, bounds, born, gone, height, width, whole):
    assets = born.shape[0]
    every = assets // TILE
    own = width // TILE
    if whole:
        mirrored = [(i, j) for j in range(every) for i in range(j)]
        plain = [(i, i) for i in range(every)]
        first = jnp.int32(0)
    else:
        mirrored = []
        plain = [(i, j) for j in range(own) for i in range(every)]
        first = (lax.axis_index("asset") * own).astype(jnp.int32)
    table_m = jnp.array(np.array(mirrored or [(0, 0)], np.int32).T)
    table_p = jnp.array(np.array(plain, np.int32).T)
    if not whole:
        table_p = table_p + jnp.stack([jnp.int32(0), first])[:, None]
    bounds = jnp.concatenate([bounds, first[None]])
    turns_m = turns_of(len(mirrored)) if mirrored else 1
    turns_p = turns_of(len(plain))
    sizes = (
        tuple(p.shape[0] for p in pieces),
        height,
        (len(mirrored) // turns_m, turns_m),
        (len(plain) // turns_p, turns_p),
        not whole,
    )
    f32, bf16 = jnp.float32, jnp.bfloat16
    vmem = pl.BlockSpec(memory_space=pltpu.VMEM)
    smem = pl.BlockSpec(memory_space=pltpu.SMEM)
    depth = SPAN
    flops = 12 * 2 * depth * TILE * TILE * (len(mirrored) + len(plain))
    return pl.pallas_call(
        functools.partial(correlation_kernel, sizes),
        out_shape=jax.ShapeDtypeStruct((assets, width), f32),
        in_specs=[vmem] * len(pieces) + [smem] * 4 + [vmem] * 2,
        out_specs=pl.BlockSpec(memory_space=pl.ANY),
        scratch_shapes=[pltpu.VMEM((depth, assets), bf16)] * 5
        + [pltpu.VMEM((assets, depth), bf16)] * 5
        + [
            pltpu.VMEM((2, 6, TILE, TILE), f32),
            pltpu.VMEM((2, turns_m, TILE, TILE), f32),
            pltpu.VMEM((2, turns_m, TILE, TILE), f32),
            pltpu.VMEM((2, turns_p, TILE, TILE), f32),
            pltpu.SemaphoreType.DMA((2, turns_m)),
            pltpu.SemaphoreType.DMA((2, turns_m)),
            pltpu.SemaphoreType.DMA((2, turns_p)),
        ],
        cost_estimate=pl.CostEstimate(flops=flops, bytes_accessed=4 * assets * width, transcendentals=assets * width),
        compiler_params=pltpu.CompilerParams(vmem_limit_bytes=56 * 2**20),
    )(*pieces, starts, bounds, table_m, table_p, born[None], gone[None])


def on_device(returns, windows, listed_from, listed_until):
    height, width = returns.shape
    members = SPAN // height // 2
    rows = lax.all_gather(returns, "asset", axis=1, tiled=True)
    pieces = gather_span(rows, "tm", members)
    starts = block_days("tm", members, height)
    after = (lax.axis_index("tm") + 1) * height
    bounds = jnp.stack([jnp.maximum(after - windows[0], 0), after]).astype(jnp.int32)
    whole = lax.axis_size("asset") == 1
    return correlation(pieces, starts, bounds, listed_from, listed_until, height, width, whole)[None]


def solution(mesh):
    placed = (P("tm", "asset"), P("tm"), P(), P())
    step = jax.shard_map(on_device, mesh=mesh, in_specs=placed, out_specs=P("tm", None, "asset"), check_vma=False)

    def call(*args):
        with jax.sharding.use_abstract_mesh(mesh.abstract_mesh):
            return step(*args)

    return call
```

```python
import dataclasses
import functools

import jax
import jax.numpy as jnp
import numpy as np
from jax import lax
from jax.experimental import pallas as pl
from jax.experimental.pallas import tpu as pltpu
from jax.sharding import PartitionSpec as P

SPAN = 256
TILE = 256
LANES = 128
UNROLL = 7
UNROLL_OWN = 4


@dataclasses.dataclass(frozen=True)
class Plan:
    pieces: int
    height: int
    width: int
    members: int
    whole: bool
    mirrored: tuple
    plain: tuple


def cycle(array, axis, by):
    devices = lax.axis_size(axis)
    return lax.ppermute(array, axis, [(i, (i + by) % devices) for i in range(devices)])


def swap(array, axis, by):
    devices = lax.axis_size(axis)
    return lax.ppermute(array, axis, [(i, i ^ by) for i in range(devices)])


def gather_span(rows, axis, members):
    member = lax.rem(lax.axis_index(axis), members)
    before = cycle(rows, axis, members)
    middle = [swap(before, axis, by) for by in range(2, members, 2)]
    before2 = cycle(before, axis, members)

    def outer(by):
        return jnp.where((member ^ by) > member, rows, before2)

    ends = [swap(outer(by), axis, by) for by in range(2, members, 2)]
    relayed = [swap(piece, axis, 1) for piece in (before, *middle, outer(1), *ends)]
    return [before, *middle, *relayed[: members // 2], rows, *ends, *relayed[members // 2 :]]


def correlation_kernel(plan, *refs):
    pieces = refs[: plan.pieces]
    window, table, born, gone, out = refs[plan.pieces : plan.pieces + 5]
    (hi, lo, sq, sl, on, low, high, sums, buf_m, buf_t, buf_p, sem_m, sem_t, sem_p) = refs[plan.pieces + 5 :]
    assets = born.shape[1]
    f32, bf16 = jnp.float32, jnp.bfloat16
    depth = plan.height * plan.pieces

    position = lax.axis_index("tm")
    member = lax.rem(position, plan.members)
    group = lax.div(position, plan.members)
    first = lax.axis_index("asset") * (plan.width // TILE)
    after = (position + 1) * plan.height
    earliest = jnp.maximum(after - window[0], 0)

    def block_start(piece):
        order = [0] + list(range(2, plan.members, 2)) + [1] + [by ^ 1 for by in range(2, plan.members, 2)]
        other = member ^ order[piece % plan.members]
        if piece < plan.members:
            source = group - 1
        else:
            source = jnp.where(other > member, group - 2, group)
        return (source * plan.members + other) * plan.height

    lane = lax.broadcasted_iota(jnp.int32, (8, depth), 1)
    days = lax.rem(lane, plan.height)
    for piece in range(plan.pieces):
        days = days + jnp.where(lax.div(lane, plan.height) == piece, block_start(piece), 0)
    days = days.astype(f32)[:1]

    def split(x):
        high_part = x.astype(bf16)
        return high_part, (x - high_part.astype(f32)).astype(bf16)

    def prepare(step, carry):
        cols = pl.ds(pl.multiple_of(step * TILE, TILE), TILE)
        begin = jnp.maximum(born[:, cols], earliest).astype(f32)
        end = jnp.minimum(gone[:, cols], after).astype(f32)
        begin = jnp.broadcast_to(begin, (LANES, TILE)).T
        end = jnp.broadcast_to(end, (LANES, TILE)).T
        low[cols, :] = begin
        high[cols, :] = end
        for part in range(0, depth, LANES):
            days_at = days[:, part : part + LANES]
            at = pl.ds(part, LANES)
            count = LANES // plan.height
            which = range(part // plan.height, part // plan.height + count)
            value = jnp.concatenate([pieces[p][:, cols] for p in which], axis=0).T
            live = (days_at >= begin) & (days_at < end)
            value = jnp.where(live, value, 0.0)
            on[cols, at] = jnp.where(live, 1.0, 0.0).astype(bf16)
            hi[cols, at], lo[cols, at] = split(value)
            sq[cols, at], sl[cols, at] = split(value * value)
        return carry

    lax.fori_loop(0, assets // TILE, prepare, 0)

    def body(*accs):
        units = accs[:4], accs[4:]
        for acc in accs:
            sums[0, 0] = pltpu.matmul_pop(acc)
        push_at = [0, 0]
        acc_at = [0, 0]

        def tile(index):
            return pl.ds(pl.multiple_of(index * TILE, TILE), TILE)

        def load(ref, j, unit):
            pltpu.matmul_push_rhs(ref[tile(j), :], staging_register=push_at[unit] % 2, mxu_index=unit, transpose=True)
            push_at[unit] += 1
            return (push_at[unit] - 1) % 2

        def fresh(unit):
            acc_at[unit] += 1
            return units[unit][(acc_at[unit] - 1) % 4]

        def add(acc, ref, i, register=None):
            pltpu.matmul_acc_lhs(acc, ref[tile(i), :], load_staged_rhs=register)

        def products(i, j, turn):
            x, y = turn % 2, 1 - turn % 2
            left, left_sq, right_sq = fresh(x), fresh(x), fresh(x)
            cross, right = fresh(y), fresh(y)
            r = load(on, j, x)
            s = load(hi, j, y)
            add(left, hi, i, r)
            add(cross, hi, i, s)
            r = load(sq, j, x)
            s = load(lo, j, y)
            add(left, lo, i)
            add(cross, lo, i)
            add(left_sq, sq, i)
            add(right, on, i)
            add(left_sq, sl, i)
            add(cross, hi, i, s)
            add(right_sq, on, i, r)
            r = load(sl, j, x)
            add(right, on, i)
            add(right_sq, on, i, r)
            for k, acc in enumerate((left, cross, left_sq, right, right_sq)):
                sums[turn % 2, k] = pltpu.matmul_pop(acc)

        def own_products(i, turn):
            x, y = turn % 2, 1 - turn % 2
            left, left_sq = fresh(x), fresh(x)
            cross = fresh(y)
            r = load(on, i, x)
            s = load(hi, i, y)
            add(left, hi, i, r)
            add(cross, hi, i, s)
            s = load(lo, i, y)
            add(left, lo, i)
            add(cross, lo, i)
            add(left_sq, sq, i)
            add(cross, hi, i, s)
            add(left_sq, sl, i)
            for k, acc in enumerate((left, cross, left_sq)):
                sums[turn % 2, k] = pltpu.matmul_pop(acc)
            sums[turn % 2, 3] = sums[turn % 2, 0].T
            sums[turn % 2, 4] = sums[turn % 2, 2].T

        def combine(i, j, turn, target, mirror):
            at = turn % 2
            step = 16
            for row in range(0, TILE, step):
                mine = pl.ds(pl.multiple_of(i * TILE + row, step), step)
                for col in range(0, TILE, LANES):
                    spot = (pl.ds(row, step), pl.ds(col, LANES))
                    theirs = pl.ds(pl.multiple_of(j * TILE + col, LANES), LANES)
                    begin = jnp.maximum(born[:, theirs], earliest).astype(f32)
                    end = jnp.minimum(gone[:, theirs], after).astype(f32)
                    pairs = jnp.maximum(jnp.minimum(high[mine, :], end) - jnp.maximum(low[mine, :], begin), 1.0)
                    left, cross, left_sq, right, right_sq = (sums[at, k, *spot] for k in range(5))
                    var_left = jnp.maximum(pairs * left_sq - left * left, pairs)
                    var_right = jnp.maximum(pairs * right_sq - right * right, pairs)
                    target[*spot] = (pairs * cross - left * right) * lax.rsqrt(var_left * var_right)
            if mirror is not None:
                mirror[...] = target[...].T

        def run(base, steps, turns, kind, buf, sem, mirror_buf, mirror_sem):
            def tiles(step):
                return [(table[0, base + step * turns + u], table[1, base + step * turns + u]) for u in range(turns)]

            def copies(step):
                slot = lax.rem(step, 2)
                for u, (i, j) in enumerate(tiles(step)):
                    yield pltpu.make_async_copy(buf.at[slot, u], out.at[tile(i), tile(j)], sem.at[slot, u])
                    if mirror_buf is not None:
                        yield pltpu.make_async_copy(mirror_buf.at[slot, u], out.at[tile(j), tile(i)], mirror_sem.at[slot, u])

            def waits(step):
                for copy in copies(step):
                    copy.wait()

            def one(step, carry):
                slot = lax.rem(step, 2)

                @pl.when(step >= 2)
                def _():
                    waits(step - 2)

                at = tiles(step)

                def finish(u):
                    i, j = at[u]
                    combine(i, j + shift, u, buf.at[slot, u], None if mirror_buf is None else mirror_buf.at[slot, u])

                shift = 0 if plan.whole else first
                for u, (i, j) in enumerate(at):
                    if kind == "own":
                        own_products(i, u)
                    else:
                        products(i, j + shift, u)
                    if u:
                        finish(u - 1)
                finish(turns - 1)
                for copy in copies(step):
                    copy.start()
                return carry

            lax.fori_loop(0, steps, one, 0)
            return lambda: [waits(step) for step in range(max(steps - 2, 0), steps)]

        ends = []
        if plan.whole:
            steps, turns = plan.mirrored
            ends.append(run(0, steps, turns, "mirror", buf_m, sem_m, buf_t, sem_t))
            ends.append(run(steps * turns, *plan.plain, "own", buf_p, sem_p, None, None))
        else:
            ends.append(run(0, *plan.plain, "plain", buf_p, sem_p, None, None))
        for end in ends:
            end()

    pl.run_scoped(body, *([pltpu.ACC(0)((TILE, TILE), f32)] * 4 + [pltpu.ACC(1)((TILE, TILE), f32)] * 4))


def turns_of(count, most):
    turns = max(t for t in range(1, most + 1) if count % t == 0)
    return count // turns, turns


def correlation(pieces, windows, born, gone, height, width, members, whole):
    assets = born.shape[0]
    every = assets // TILE
    own = width // TILE
    if whole:
        mirrored = [(i, j) for j in range(every) for i in range(j)]
        plain = [(i, i) for i in range(every)]
    else:
        mirrored = []
        plain = [(i, j) for j in range(own) for i in range(every)]
    plan = Plan(
        pieces=len(pieces),
        height=height,
        width=width,
        members=members,
        whole=whole,
        mirrored=turns_of(len(mirrored), UNROLL) if mirrored else (0, 1),
        plain=turns_of(len(plain), UNROLL_OWN),
    )
    table = jnp.array(np.array(mirrored + plain, np.int32).T)
    turns_m, turns_p = plan.mirrored[1], plan.plain[1]
    f32, bf16 = jnp.float32, jnp.bfloat16
    vmem = pl.BlockSpec(memory_space=pltpu.VMEM)
    smem = pl.BlockSpec(memory_space=pltpu.SMEM)
    depth = len(pieces) * height
    flops = 2 * depth * TILE * TILE * (11 * len(mirrored) + (7 if whole else 11) * len(plain))
    return pl.pallas_call(
        functools.partial(correlation_kernel, plan),
        out_shape=jax.ShapeDtypeStruct((assets, width), f32),
        in_specs=[vmem] * len(pieces) + [smem] * 2 + [vmem] * 2,
        out_specs=pl.BlockSpec(memory_space=pl.ANY),
        scratch_shapes=[pltpu.VMEM((assets, depth), bf16)] * 5
        + [pltpu.VMEM((assets, LANES), f32)] * 2
        + [
            pltpu.VMEM((2, 5, TILE, TILE), f32),
            pltpu.VMEM((2, turns_m, TILE, TILE), f32),
            pltpu.VMEM((2, turns_m, TILE, TILE), f32),
            pltpu.VMEM((2, turns_p, TILE, TILE), f32),
            pltpu.SemaphoreType.DMA((2, turns_m)),
            pltpu.SemaphoreType.DMA((2, turns_m)),
            pltpu.SemaphoreType.DMA((2, turns_p)),
        ],
        cost_estimate=pl.CostEstimate(flops=flops, bytes_accessed=4 * assets * width, transcendentals=assets * width),
        compiler_params=pltpu.CompilerParams(vmem_limit_bytes=56 * 2**20),
        name="correlation",
    )(*pieces, windows, table, born[None], gone[None])


def on_device(returns, windows, listed_from, listed_until):
    height, width = returns.shape
    members = SPAN // height // 2
    rows = lax.all_gather(returns, "asset", axis=1, tiled=True)
    pieces = gather_span(rows, "tm", members)
    whole = lax.axis_size("asset") == 1
    return correlation(pieces, windows, listed_from, listed_until, height, width, members, whole)[None]


def solution(mesh):
    placed = (P("tm", "asset"), P("tm"), P(), P())
    step = jax.shard_map(on_device, mesh=mesh, in_specs=placed, out_specs=P("tm", None, "asset"), check_vma=False)

    def call(*args):
        with jax.sharding.use_abstract_mesh(mesh.abstract_mesh):
            return step(*args)

    return call
```

```python
import dataclasses
import functools

import jax
import jax.numpy as jnp
from jax import lax
from jax.experimental import pallas as pl
from jax.experimental.pallas import tpu as pltpu
from jax.sharding import PartitionSpec as P

SPAN = 256
TILE = 256
LANES = 128
UNROLL = 7
UNROLL_OWN = 4


@dataclasses.dataclass(frozen=True)
class Plan:
    pieces: int
    height: int
    width: int
    members: int
    whole: bool
    mirrored: tuple
    plain: tuple


def cycle(array, axis, by):
    devices = lax.axis_size(axis)
    return lax.ppermute(array, axis, [(i, (i + by) % devices) for i in range(devices)])


def swap(array, axis, by):
    devices = lax.axis_size(axis)
    return lax.ppermute(array, axis, [(i, i ^ by) for i in range(devices)])


def gather_span(rows, axis, members, early):
    member = lax.rem(lax.axis_index(axis), members)
    before, *early = lax.optimization_barrier((cycle(rows, axis, members), *early))
    middle = [swap(before, axis, by) for by in range(2, members, 2)]
    before2 = cycle(rows, axis, 2 * members)

    def outer(by):
        return jnp.where((member ^ by) >= member, rows, before2)

    ends = [swap(outer(by), axis, by) for by in range(2, members, 2)]
    relayed = [swap(piece, axis, 1) for piece in (before, *middle, outer(1), *ends)]
    own = jnp.where(member >= 0, rows, before2)
    return [before, *middle, *relayed[: members // 2], own, *ends, *relayed[members // 2 :]], early


def correlation_kernel(plan, *refs):
    pieces = refs[: plan.pieces]
    begins, ends_at, out = refs[plan.pieces : plan.pieces + 3]
    (hi, lo, sq, sl, on, low, high, sums, buf_m, buf_t, buf_p, sem_m, sem_t, sem_p) = refs[plan.pieces + 3 :]
    assets = begins.shape[1]
    f32, bf16 = jnp.float32, jnp.bfloat16
    depth = plan.height * plan.pieces

    position = lax.axis_index("tm")
    member = lax.rem(position, plan.members)
    group = lax.div(position, plan.members)
    first = lax.axis_index("asset") * (plan.width // TILE)

    def block_start(piece):
        order = [0] + list(range(2, plan.members, 2)) + [1] + [by ^ 1 for by in range(2, plan.members, 2)]
        other = member ^ order[piece % plan.members]
        if piece < plan.members:
            source = group - 1
        else:
            source = jnp.where(other > member, group - 2, group)
        return (source * plan.members + other) * plan.height

    lane = lax.broadcasted_iota(jnp.int32, (8, depth), 1)
    days = lax.rem(lane, plan.height)
    for piece in range(plan.pieces):
        days = days + jnp.where(lax.div(lane, plan.height) == piece, block_start(piece), 0)
    days = days.astype(f32)[:1]

    def split(x):
        high_part = x.astype(bf16)
        return high_part, (x - high_part.astype(f32)).astype(bf16)

    def prepare(step, carry):
        cols = pl.ds(pl.multiple_of(step * TILE, TILE), TILE)
        begin = jnp.broadcast_to(begins[:, cols], (LANES, TILE)).T
        end = jnp.broadcast_to(ends_at[:, cols], (LANES, TILE)).T
        low[cols, :] = begin
        high[cols, :] = end
        for part in range(0, depth, LANES):
            days_at = days[:, part : part + LANES]
            at = pl.ds(part, LANES)
            count = LANES // plan.height
            which = range(part // plan.height, part // plan.height + count)
            value = jnp.concatenate([pieces[p][:, cols] for p in which], axis=0).T
            live = (days_at >= begin) & (days_at < end)
            value = jnp.where(live, value, 0.0)
            on[cols, at] = jnp.where(live, 1.0, 0.0).astype(bf16)
            hi[cols, at], lo[cols, at] = split(value)
            sq[cols, at], sl[cols, at] = split(value * value)
        return carry

    lax.fori_loop(0, assets // TILE, prepare, 0)

    def body(*accs):
        units = accs[:4], accs[4:]
        for acc in accs:
            sums[0, 0] = pltpu.matmul_pop(acc)
        push_at = [0, 0]
        acc_at = [0, 0]

        def tile(index):
            return pl.ds(pl.multiple_of(index * TILE, TILE), TILE)

        def load(ref, j, unit):
            pltpu.matmul_push_rhs(ref[tile(j), :], staging_register=push_at[unit] % 2, mxu_index=unit, transpose=True)
            push_at[unit] += 1
            return (push_at[unit] - 1) % 2

        def fresh(unit):
            acc_at[unit] += 1
            return units[unit][(acc_at[unit] - 1) % 4]

        def add(acc, ref, i, register=None):
            pltpu.matmul_acc_lhs(acc, ref[tile(i), :], load_staged_rhs=register)

        def products(i, j, turn):
            x, y = turn % 2, 1 - turn % 2
            left, left_sq, right_sq = fresh(x), fresh(x), fresh(x)
            cross, right = fresh(y), fresh(y)
            r = load(on, j, x)
            s = load(hi, j, y)
            add(left, hi, i, r)
            add(cross, hi, i, s)
            r = load(sq, j, x)
            s = load(lo, j, y)
            add(left, lo, i)
            add(cross, lo, i)
            add(left_sq, sq, i)
            add(right, on, i)
            add(left_sq, sl, i)
            add(cross, hi, i, s)
            add(right_sq, on, i, r)
            r = load(sl, j, x)
            add(right, on, i)
            add(right_sq, on, i, r)
            for k, acc in enumerate((left, cross, left_sq, right, right_sq)):
                sums[turn % 2, k] = pltpu.matmul_pop(acc)

        def own_products(i, turn):
            x, y = turn % 2, 1 - turn % 2
            left, left_sq = fresh(x), fresh(x)
            cross = fresh(y)
            r = load(on, i, x)
            s = load(hi, i, y)
            add(left, hi, i, r)
            add(cross, hi, i, s)
            s = load(lo, i, y)
            add(left, lo, i)
            add(cross, lo, i)
            add(left_sq, sq, i)
            add(cross, hi, i, s)
            add(left_sq, sl, i)
            for k, acc in enumerate((left, cross, left_sq)):
                sums[turn % 2, k] = pltpu.matmul_pop(acc)
            sums[turn % 2, 3] = sums[turn % 2, 0].T
            sums[turn % 2, 4] = sums[turn % 2, 2].T

        def combine(i, j, turn, target, mirror):
            at = turn % 2
            step = 16
            for row in range(0, TILE, step):
                mine = pl.ds(pl.multiple_of(i * TILE + row, step), step)
                for col in range(0, TILE, LANES):
                    spot = (pl.ds(row, step), pl.ds(col, LANES))
                    theirs = pl.ds(pl.multiple_of(j * TILE + col, LANES), LANES)
                    begin, end = begins[:, theirs], ends_at[:, theirs]
                    pairs = jnp.maximum(jnp.minimum(high[mine, :], end) - jnp.maximum(low[mine, :], begin), 1.0)
                    left, cross, left_sq, right, right_sq = (sums[at, k, *spot] for k in range(5))
                    var_left = jnp.maximum(pairs * left_sq - left * left, pairs)
                    var_right = jnp.maximum(pairs * right_sq - right * right, pairs)
                    target[*spot] = (pairs * cross - left * right) * lax.rsqrt(var_left * var_right)
            if mirror is not None:
                mirror[...] = target[...].T

        def tile_at(kind, index):
            index = jnp.int32(index)
            if kind == "own":
                return index, index
            if kind == "plain":
                return lax.rem(index, assets // TILE), lax.div(index, assets // TILE)
            column = jnp.int32(1)
            for j in range(2, assets // TILE):
                column = column + (index >= j * (j - 1) // 2).astype(jnp.int32)
            return index - lax.div(column * (column - 1), 2), column

        def run(steps, turns, kind, buf, sem, mirror_buf, mirror_sem):
            def tiles(step):
                return [tile_at(kind, step * turns + u) for u in range(turns)]

            def copies(step):
                slot = lax.rem(step, 2)
                for u, (i, j) in enumerate(tiles(step)):
                    yield pltpu.make_async_copy(buf.at[slot, u], out.at[tile(i), tile(j)], sem.at[slot, u])
                    if mirror_buf is not None:
                        yield pltpu.make_async_copy(mirror_buf.at[slot, u], out.at[tile(j), tile(i)], mirror_sem.at[slot, u])

            def waits(step):
                for copy in copies(step):
                    copy.wait()

            def one(step, carry):
                slot = lax.rem(step, 2)

                @pl.when(step >= 2)
                def _():
                    waits(step - 2)

                at = tiles(step)

                def finish(u):
                    i, j = at[u]
                    combine(i, j + shift, u, buf.at[slot, u], None if mirror_buf is None else mirror_buf.at[slot, u])

                shift = 0 if plan.whole else first
                for u, (i, j) in enumerate(at):
                    if kind == "own":
                        own_products(i, u)
                    else:
                        products(i, j + shift, u)
                    if u:
                        finish(u - 1)
                finish(turns - 1)
                for copy in copies(step):
                    copy.start()
                return carry

            lax.fori_loop(0, steps, one, 0)
            return lambda: [waits(step) for step in range(max(steps - 2, 0), steps)]

        ends = []
        if plan.whole:
            ends.append(run(*plan.mirrored, "mirror", buf_m, sem_m, buf_t, sem_t))
            ends.append(run(*plan.plain, "own", buf_p, sem_p, None, None))
        else:
            ends.append(run(*plan.plain, "plain", buf_p, sem_p, None, None))
        for end in ends:
            end()

    pl.run_scoped(body, *([pltpu.ACC(0)((TILE, TILE), f32)] * 4 + [pltpu.ACC(1)((TILE, TILE), f32)] * 4))


def turns_of(count, most):
    turns = max(t for t in range(1, most + 1) if count % t == 0)
    return count // turns, turns


def correlation(pieces, begins, ends, height, width, members, whole):
    assets = begins.shape[1]
    every = assets // TILE
    own = width // TILE
    mirrored = every * (every - 1) // 2 if whole else 0
    plain = every if whole else every * own
    plan = Plan(
        pieces=len(pieces),
        height=height,
        width=width,
        members=members,
        whole=whole,
        mirrored=turns_of(mirrored, UNROLL) if mirrored else (0, 1),
        plain=turns_of(plain, UNROLL_OWN),
    )
    turns_m, turns_p = plan.mirrored[1], plan.plain[1]
    f32, bf16 = jnp.float32, jnp.bfloat16
    vmem = pl.BlockSpec(memory_space=pltpu.VMEM)
    depth = len(pieces) * height
    flops = 2 * depth * TILE * TILE * (11 * mirrored + (7 if whole else 11) * plain)
    return pl.pallas_call(
        functools.partial(correlation_kernel, plan),
        out_shape=jax.ShapeDtypeStruct((assets, width), f32),
        in_specs=[vmem] * (len(pieces) + 2),
        out_specs=pl.BlockSpec(memory_space=pl.ANY),
        scratch_shapes=[pltpu.VMEM((assets, depth), bf16)] * 5
        + [pltpu.VMEM((assets, LANES), f32)] * 2
        + [
            pltpu.VMEM((2, 5, TILE, TILE), f32),
            pltpu.VMEM((2, turns_m, TILE, TILE), f32),
            pltpu.VMEM((2, turns_m, TILE, TILE), f32),
            pltpu.VMEM((2, turns_p, TILE, TILE), f32),
            pltpu.SemaphoreType.DMA((2, turns_m)),
            pltpu.SemaphoreType.DMA((2, turns_m)),
            pltpu.SemaphoreType.DMA((2, turns_p)),
        ],
        cost_estimate=pl.CostEstimate(flops=flops, bytes_accessed=4 * assets * width, transcendentals=assets * width),
        compiler_params=pltpu.CompilerParams(vmem_limit_bytes=32 * 2**20),
        name="correlation",
    )(*pieces, begins, ends)


def on_device(returns, windows, listed_from, listed_until):
    height, width = returns.shape
    members = SPAN // height // 2
    rows = lax.all_gather(returns, "asset", axis=1, tiled=True)
    after = (lax.axis_index("tm") + 1) * height
    earliest = jnp.maximum(after - windows[0], 0)
    begins = jnp.maximum(listed_from, earliest).astype(jnp.float32)[None]
    ends = jnp.minimum(listed_until, after).astype(jnp.float32)[None]
    pieces, (begins, ends) = gather_span(rows, "tm", members, (begins, ends))
    whole = lax.axis_size("asset") == 1
    return correlation(pieces, begins, ends, height, width, members, whole)[None]


def solution(mesh):
    placed = (P("tm", "asset"), P("tm"), P(), P())
    step = jax.shard_map(on_device, mesh=mesh, in_specs=placed, out_specs=P("tm", None, "asset"), check_vma=False)

    def call(*args):
        with jax.sharding.use_abstract_mesh(mesh.abstract_mesh):
            return step(*args)

    return call
```

```python
import dataclasses
import functools

import jax
import jax.numpy as jnp
from jax import lax
from jax.experimental import pallas as pl
from jax.experimental.pallas import tpu as pltpu
from jax.sharding import PartitionSpec as P

SPAN = 256
TILE = 256
LANES = 128
UNROLL = 4
UNROLL_OWN = 4


@dataclasses.dataclass(frozen=True)
class Plan:
    pieces: int
    height: int
    width: int
    members: int
    whole: bool
    mirrored: tuple
    plain: tuple


def cycle(array, axis, by):
    devices = lax.axis_size(axis)
    return lax.ppermute(array, axis, [(i, (i + by) % devices) for i in range(devices)])


def swap(array, axis, by):
    devices = lax.axis_size(axis)
    return lax.ppermute(array, axis, [(i, i ^ by) for i in range(devices)])


def gather_span(rows, axis, members, early):
    member = lax.rem(lax.axis_index(axis), members)
    before, *early = lax.optimization_barrier((cycle(rows, axis, members), *early))
    middle = [swap(before, axis, by) for by in range(2, members, 2)]
    before2 = cycle(rows, axis, 2 * members)

    def outer(by):
        return jnp.where((member ^ by) >= member, rows, before2)

    ends = [swap(outer(by), axis, by) for by in range(2, members, 2)]
    relayed = [swap(piece, axis, 1) for piece in (before, *middle, outer(1), *ends)]
    own = jnp.where(member >= 0, rows, before2)
    return [before, *middle, *relayed[: members // 2], own, *ends, *relayed[members // 2 :]], early


def correlation_kernel(plan, *refs):
    pieces = refs[: plan.pieces]
    begins, ends_at, out = refs[plan.pieces : plan.pieces + 3]
    (hi, lo, sq, sl, on, low, high, sums, buf_m, buf_t, buf_p, buf_e, sem_m, sem_t, sem_p, sem_e) = refs[plan.pieces + 3 :]
    assets = begins.shape[1]
    f32, bf16 = jnp.float32, jnp.bfloat16
    depth = plan.height * plan.pieces

    position = lax.axis_index("tm")
    member = lax.rem(position, plan.members)
    group = lax.div(position, plan.members)
    first = lax.axis_index("asset") * (plan.width // TILE)

    def block_start(piece):
        order = [0] + list(range(2, plan.members, 2)) + [1] + [by ^ 1 for by in range(2, plan.members, 2)]
        other = member ^ order[piece % plan.members]
        if piece < plan.members:
            source = group - 1
        else:
            source = jnp.where(other > member, group - 2, group)
        return (source * plan.members + other) * plan.height

    lane = lax.broadcasted_iota(jnp.int32, (8, depth), 1)
    days = lax.rem(lane, plan.height)
    for piece in range(plan.pieces):
        days = days + jnp.where(lax.div(lane, plan.height) == piece, block_start(piece), 0)
    days = days.astype(f32)[:1]

    def split(x):
        high_part = x.astype(bf16)
        return high_part, (x - high_part.astype(f32)).astype(bf16)

    def prepare(step, carry):
        cols = pl.ds(pl.multiple_of(step * TILE, TILE), TILE)
        begin = jnp.broadcast_to(begins[:, cols], (LANES, TILE)).T
        end = jnp.broadcast_to(ends_at[:, cols], (LANES, TILE)).T
        low[cols, :] = begin
        high[cols, :] = end
        for part in range(0, depth, LANES):
            days_at = days[:, part : part + LANES]
            at = pl.ds(part, LANES)
            count = LANES // plan.height
            which = range(part // plan.height, part // plan.height + count)
            value = jnp.concatenate([pieces[p][:, cols] for p in which], axis=0).T
            live = (days_at >= begin) & (days_at < end)
            value = jnp.where(live, value, 0.0)
            on[cols, at] = jnp.where(live, 1.0, 0.0).astype(bf16)
            hi[cols, at], lo[cols, at] = split(value)
            sq[cols, at], sl[cols, at] = split(value * value)
        return carry

    lax.fori_loop(0, assets // TILE, prepare, 0)

    def body(*accs):
        units = accs[:4], accs[4:]
        for acc in accs:
            sums[0, 0] = pltpu.matmul_pop(acc)
        push_at = [0, 0]
        acc_at = [0, 0]

        def tile(index):
            return pl.ds(pl.multiple_of(index * TILE, TILE), TILE)

        def load(ref, j, unit):
            pltpu.matmul_push_rhs(ref[tile(j), :], staging_register=push_at[unit] % 2, mxu_index=unit, transpose=True)
            push_at[unit] += 1
            return (push_at[unit] - 1) % 2

        def fresh(unit):
            acc_at[unit] += 1
            return units[unit][(acc_at[unit] - 1) % 4]

        def add(acc, ref, i, register=None):
            pltpu.matmul_acc_lhs(acc, ref[tile(i), :], load_staged_rhs=register)

        def slot_of(turn, last):
            return 2 if last else turn % 2

        def products(i, j, turn, last=False):
            x, y = turn % 2, 1 - turn % 2
            left, left_sq, right_sq = fresh(x), fresh(x), fresh(x)
            cross, right = fresh(y), fresh(y)
            r = load(on, j, x)
            s = load(hi, j, y)
            add(left, hi, i, r)
            add(cross, hi, i, s)
            r = load(sq, j, x)
            s = load(lo, j, y)
            add(left, lo, i)
            add(cross, lo, i)
            add(left_sq, sq, i)
            add(right, on, i)
            add(left_sq, sl, i)
            add(cross, hi, i, s)
            add(right_sq, on, i, r)
            r = load(sl, j, x)
            add(right, on, i)
            add(right_sq, on, i, r)
            for k, acc in enumerate((left, cross, left_sq, right, right_sq)):
                sums[slot_of(turn, last), k] = pltpu.matmul_pop(acc)

        def own_products(i, turn):
            x, y = turn % 2, 1 - turn % 2
            left, left_sq = fresh(x), fresh(x)
            cross = fresh(y)
            r = load(on, i, x)
            s = load(hi, i, y)
            add(left, hi, i, r)
            add(cross, hi, i, s)
            s = load(lo, i, y)
            add(left, lo, i)
            add(cross, lo, i)
            add(left_sq, sq, i)
            add(cross, hi, i, s)
            add(left_sq, sl, i)
            for k, acc in enumerate((left, cross, left_sq)):
                sums[turn % 2, k] = pltpu.matmul_pop(acc)
            sums[turn % 2, 3] = sums[turn % 2, 0].T
            sums[turn % 2, 4] = sums[turn % 2, 2].T

        def combine(i, j, at, target, mirror):
            step = 16
            for row in range(0, TILE, step):
                mine = pl.ds(pl.multiple_of(i * TILE + row, step), step)
                for col in range(0, TILE, LANES):
                    spot = (pl.ds(row, step), pl.ds(col, LANES))
                    theirs = pl.ds(pl.multiple_of(j * TILE + col, LANES), LANES)
                    begin, end = begins[:, theirs], ends_at[:, theirs]
                    pairs = jnp.maximum(jnp.minimum(high[mine, :], end) - jnp.maximum(low[mine, :], begin), 1.0)
                    left, cross, left_sq, right, right_sq = (sums[at, k, *spot] for k in range(5))
                    var_left = jnp.maximum(pairs * left_sq - left * left, pairs)
                    var_right = jnp.maximum(pairs * right_sq - right * right, pairs)
                    target[*spot] = (pairs * cross - left * right) * lax.rsqrt(var_left * var_right)
            if mirror is not None:
                mirror[...] = target[...].T

        def tile_at(kind, index):
            index = jnp.int32(index)
            if kind == "own":
                return index, index
            if kind == "plain":
                return lax.rem(index, assets // TILE), lax.div(index, assets // TILE)
            column = jnp.int32(1)
            for j in range(2, assets // TILE):
                column = column + (index >= j * (j - 1) // 2).astype(jnp.int32)
            return index - lax.div(column * (column - 1), 2), column

        def run(steps, turns, kind, buf, sem, mirror_buf, mirror_sem):
            def tiles(step):
                return [tile_at(kind, step * turns + u) for u in range(turns)]

            def copies(step):
                slot = lax.rem(step, 2)
                for u, (i, j) in enumerate(tiles(step)):
                    yield pltpu.make_async_copy(buf.at[slot, u], out.at[tile(i), tile(j)], sem.at[slot, u])
                    if mirror_buf is not None:
                        yield pltpu.make_async_copy(mirror_buf.at[slot, u], out.at[tile(j), tile(i)], mirror_sem.at[slot, u])

            def waits(step):
                for copy in copies(step):
                    copy.wait()

            def one(step, carry):
                slot = lax.rem(step, 2)

                @pl.when(step >= 2)
                def _():
                    waits(step - 2)

                at = tiles(step)

                def finish(u):
                    i, j = at[u]
                    combine(i, j + shift, u % 2, buf.at[slot, u], None if mirror_buf is None else mirror_buf.at[slot, u])

                shift = 0 if plan.whole else first
                for u, (i, j) in enumerate(at):
                    if kind == "own":
                        own_products(i, u)
                    else:
                        products(i, j + shift, u)
                    if u:
                        finish(u - 1)
                finish(turns - 1)
                for copy in copies(step):
                    copy.start()
                return carry

            lax.fori_loop(0, steps, one, 0)
            return lambda: [waits(step) for step in range(max(steps - 2, 0), steps)]

        def run_lagged(steps, turns, kind):
            final = steps * turns - 1

            def tiles(step):
                lagging = jnp.where(step == 0, final, step * turns - 1)
                return [tile_at(kind, lagging)] + [tile_at(kind, step * turns + u) for u in range(turns)]

            def pair(i, j, source, mirror, sem, mirror_sem):
                yield pltpu.make_async_copy(source, out.at[tile(i), tile(j)], sem)
                yield pltpu.make_async_copy(mirror, out.at[tile(j), tile(i)], mirror_sem)

            def copies(step):
                slot = lax.rem(step, 2)
                for u, (i, j) in enumerate(tiles(step)[:turns]):
                    yield from pair(i, j, buf_m.at[slot, u], buf_t.at[slot, u], sem_m.at[slot, u], sem_t.at[slot, u])

            def waits(step):
                for copy in copies(step):
                    copy.wait()

            def one(step, carry):
                slot = lax.rem(step, 2)

                @pl.when(step >= 2)
                def _():
                    waits(step - 2)

                at = tiles(step)
                for u in range(turns):
                    products(*at[u + 1], u, last=u == turns - 1)
                    combine(*at[u], slot_of(u - 1, u == 0), buf_m.at[slot, u], buf_t.at[slot, u])
                for copy in copies(step):
                    copy.start()
                return carry

            lax.fori_loop(0, steps, one, 0)
            i, j = tile_at(kind, final)
            combine(i, j, 2, buf_e.at[0], buf_e.at[1])
            rest = list(pair(i, j, buf_e.at[0], buf_e.at[1], sem_e.at[0], sem_e.at[1]))
            for copy in rest:
                copy.start()

            def end():
                for step in range(max(steps - 2, 0), steps):
                    waits(step)
                for copy in rest:
                    copy.wait()

            return end

        ends = []
        if plan.whole:
            if plan.mirrored[0] > 2:
                ends.append(run_lagged(*plan.mirrored, "mirror"))
            else:
                ends.append(run(*plan.mirrored, "mirror", buf_m, sem_m, buf_t, sem_t))
            ends.append(run(*plan.plain, "own", buf_p, sem_p, None, None))
        else:
            ends.append(run(*plan.plain, "plain", buf_p, sem_p, None, None))
        for end in ends:
            end()

    pl.run_scoped(body, *([pltpu.ACC(0)((TILE, TILE), f32)] * 4 + [pltpu.ACC(1)((TILE, TILE), f32)] * 4))


def turns_of(count, most):
    turns = max(t for t in range(1, most + 1) if count % t == 0)
    return count // turns, turns


def correlation(pieces, begins, ends, height, width, members, whole):
    assets = begins.shape[1]
    every = assets // TILE
    own = width // TILE
    mirrored = every * (every - 1) // 2 if whole else 0
    plain = every if whole else every * own
    plan = Plan(
        pieces=len(pieces),
        height=height,
        width=width,
        members=members,
        whole=whole,
        mirrored=turns_of(mirrored, UNROLL) if mirrored else (0, 1),
        plain=turns_of(plain, UNROLL_OWN),
    )
    turns_m, turns_p = plan.mirrored[1], plan.plain[1]
    f32, bf16 = jnp.float32, jnp.bfloat16
    vmem = pl.BlockSpec(memory_space=pltpu.VMEM)
    depth = len(pieces) * height
    flops = 2 * depth * TILE * TILE * (11 * mirrored + (7 if whole else 11) * plain)
    return pl.pallas_call(
        functools.partial(correlation_kernel, plan),
        out_shape=jax.ShapeDtypeStruct((assets, width), f32),
        in_specs=[vmem] * (len(pieces) + 2),
        out_specs=pl.BlockSpec(memory_space=pl.ANY),
        scratch_shapes=[pltpu.VMEM((assets, depth), bf16)] * 5
        + [pltpu.VMEM((assets, LANES), f32)] * 2
        + [
            pltpu.VMEM((3, 5, TILE, TILE), f32),
            pltpu.VMEM((2, turns_m, TILE, TILE), f32),
            pltpu.VMEM((2, turns_m, TILE, TILE), f32),
            pltpu.VMEM((2, turns_p, TILE, TILE), f32),
            pltpu.VMEM((2, TILE, TILE), f32),
            pltpu.SemaphoreType.DMA((2, turns_m)),
            pltpu.SemaphoreType.DMA((2, turns_m)),
            pltpu.SemaphoreType.DMA((2, turns_p)),
            pltpu.SemaphoreType.DMA((2,)),
        ],
        cost_estimate=pl.CostEstimate(flops=flops, bytes_accessed=4 * assets * width, transcendentals=assets * width),
        compiler_params=pltpu.CompilerParams(vmem_limit_bytes=32 * 2**20),
        name="correlation",
    )(*pieces, begins, ends)


def on_device(returns, windows, listed_from, listed_until):
    height, width = returns.shape
    members = SPAN // height // 2
    rows = lax.all_gather(returns, "asset", axis=1, tiled=True)
    after = (lax.axis_index("tm") + 1) * height
    earliest = jnp.maximum(after - windows[0], 0)
    begins = jnp.maximum(listed_from, earliest).astype(jnp.float32)[None]
    ends = jnp.minimum(listed_until, after).astype(jnp.float32)[None]
    pieces, (begins, ends) = gather_span(rows, "tm", members, (begins, ends))
    whole = lax.axis_size("asset") == 1
    return correlation(pieces, begins, ends, height, width, members, whole)[None]


def solution(mesh):
    placed = (P("tm", "asset"), P("tm"), P(), P())
    step = jax.shard_map(on_device, mesh=mesh, in_specs=placed, out_specs=P("tm", None, "asset"), check_vma=False)

    def call(*args):
        with jax.sharding.use_abstract_mesh(mesh.abstract_mesh):
            return step(*args)

    return call
```

```python
import dataclasses
import functools

import jax
import jax.numpy as jnp
from jax import lax
from jax.experimental import pallas as pl
from jax.experimental.pallas import tpu as pltpu
from jax.sharding import PartitionSpec as P

SPAN = 256
TILE = 256
LANES = 128
UNROLL = 4
UNROLL_OWN = 4


@dataclasses.dataclass(frozen=True)
class Plan:
    pieces: int
    height: int
    width: int
    members: int
    whole: bool
    mirrored: tuple
    plain: tuple


def cycle(array, axis, by):
    devices = lax.axis_size(axis)
    return lax.ppermute(array, axis, [(i, (i + by) % devices) for i in range(devices)])


def swap(array, axis, by):
    devices = lax.axis_size(axis)
    return lax.ppermute(array, axis, [(i, i ^ by) for i in range(devices)])


def gather_span(rows, axis, members, early):
    member = lax.rem(lax.axis_index(axis), members)
    own = jnp.where(member >= 0, rows, 0.0)
    before, own, *early = lax.optimization_barrier((cycle(rows, axis, members), own, *early))
    middle = [swap(before, axis, by) for by in range(2, members, 2)]
    before2 = cycle(rows, axis, 2 * members)

    def outer(by):
        return jnp.where((member ^ by) >= member, own, before2)

    ends = [swap(outer(by), axis, by) for by in range(2, members, 2)]
    relayed = [swap(piece, axis, 1) for piece in (before, *middle, outer(1), *ends)]
    return [before, *middle, *relayed[: members // 2], own, *ends, *relayed[members // 2 :]], early


def correlation_kernel(plan, *refs):
    pieces = refs[: plan.pieces]
    begins, ends_at, out = refs[plan.pieces : plan.pieces + 3]
    (hi, lo, sq, sl, on, low, high, sums, buf_m, buf_t, buf_p, buf_e, sem_m, sem_t, sem_p, sem_e) = refs[plan.pieces + 3 :]
    assets = begins.shape[1]
    f32, bf16 = jnp.float32, jnp.bfloat16
    depth = plan.height * plan.pieces

    position = lax.axis_index("tm")
    member = lax.rem(position, plan.members)
    group = lax.div(position, plan.members)
    first = lax.axis_index("asset") * (plan.width // TILE)

    def block_start(piece):
        order = [0] + list(range(2, plan.members, 2)) + [1] + [by ^ 1 for by in range(2, plan.members, 2)]
        other = member ^ order[piece % plan.members]
        if piece < plan.members:
            source = group - 1
        else:
            source = jnp.where(other > member, group - 2, group)
        return (source * plan.members + other) * plan.height

    lane = lax.broadcasted_iota(jnp.int32, (8, depth), 1)
    days = lax.rem(lane, plan.height)
    for piece in range(plan.pieces):
        days = days + jnp.where(lax.div(lane, plan.height) == piece, block_start(piece), 0)
    days = days.astype(f32)[:1]

    def split(x):
        high_part = x.astype(bf16)
        return high_part, (x - high_part.astype(f32)).astype(bf16)

    def prepare(step, carry):
        cols = pl.ds(pl.multiple_of(step * TILE, TILE), TILE)
        begin = jnp.broadcast_to(begins[:, cols], (LANES, TILE)).T
        end = jnp.broadcast_to(ends_at[:, cols], (LANES, TILE)).T
        low[cols, :] = begin
        high[cols, :] = end
        for part in range(0, depth, LANES):
            days_at = days[:, part : part + LANES]
            at = pl.ds(part, LANES)
            count = LANES // plan.height
            which = range(part // plan.height, part // plan.height + count)
            value = jnp.concatenate([pieces[p][:, cols] for p in which], axis=0).T
            live = (days_at >= begin) & (days_at < end)
            value = jnp.where(live, value, 0.0)
            on[cols, at] = jnp.where(live, 1.0, 0.0).astype(bf16)
            hi[cols, at], lo[cols, at] = split(value)
            sq[cols, at], sl[cols, at] = split(value * value)
        return carry

    lax.fori_loop(0, assets // TILE, prepare, 0)

    def body(*accs):
        units = accs[:4], accs[4:]
        for acc in accs:
            sums[0, 0] = pltpu.matmul_pop(acc)
        push_at = [0, 0]
        acc_at = [0, 0]

        def tile(index):
            return pl.ds(pl.multiple_of(index * TILE, TILE), TILE)

        def load(ref, j, unit):
            pltpu.matmul_push_rhs(ref[tile(j), :], staging_register=push_at[unit] % 2, mxu_index=unit, transpose=True)
            push_at[unit] += 1
            return (push_at[unit] - 1) % 2

        def fresh(unit):
            acc_at[unit] += 1
            return units[unit][(acc_at[unit] - 1) % 4]

        def add(acc, ref, i, register=None):
            pltpu.matmul_acc_lhs(acc, ref[tile(i), :], load_staged_rhs=register)

        def slot_of(turn, last):
            return 2 if last else turn % 2

        def products(i, j, turn, last=False):
            x, y = turn % 2, 1 - turn % 2
            left, left_sq, right_sq = fresh(x), fresh(x), fresh(x)
            cross, right = fresh(y), fresh(y)
            r = load(on, j, x)
            s = load(hi, j, y)
            add(left, hi, i, r)
            add(cross, hi, i, s)
            r = load(sq, j, x)
            s = load(lo, j, y)
            add(left, lo, i)
            add(cross, lo, i)
            add(left_sq, sq, i)
            add(right, on, i)
            add(left_sq, sl, i)
            add(cross, hi, i, s)
            add(right_sq, on, i, r)
            r = load(sl, j, x)
            add(right, on, i)
            add(right_sq, on, i, r)
            for k, acc in enumerate((left, cross, left_sq, right, right_sq)):
                sums[slot_of(turn, last), k] = pltpu.matmul_pop(acc)

        def own_products(i, turn):
            x, y = turn % 2, 1 - turn % 2
            left, left_sq = fresh(x), fresh(x)
            cross = fresh(y)
            r = load(on, i, x)
            s = load(hi, i, y)
            add(left, hi, i, r)
            add(cross, hi, i, s)
            s = load(lo, i, y)
            add(left, lo, i)
            add(cross, lo, i)
            add(left_sq, sq, i)
            add(cross, hi, i, s)
            add(left_sq, sl, i)
            for k, acc in enumerate((left, cross, left_sq)):
                sums[turn % 2, k] = pltpu.matmul_pop(acc)
            sums[turn % 2, 3] = sums[turn % 2, 0].T
            sums[turn % 2, 4] = sums[turn % 2, 2].T

        def combine(i, j, at, target, mirror):
            step = 16
            for row in range(0, TILE, step):
                mine = pl.ds(pl.multiple_of(i * TILE + row, step), step)
                for col in range(0, TILE, LANES):
                    spot = (pl.ds(row, step), pl.ds(col, LANES))
                    theirs = pl.ds(pl.multiple_of(j * TILE + col, LANES), LANES)
                    begin, end = begins[:, theirs], ends_at[:, theirs]
                    pairs = jnp.maximum(jnp.minimum(high[mine, :], end) - jnp.maximum(low[mine, :], begin), 1.0)
                    left, cross, left_sq, right, right_sq = (sums[at, k, *spot] for k in range(5))
                    var_left = jnp.maximum(pairs * left_sq - left * left, pairs)
                    var_right = jnp.maximum(pairs * right_sq - right * right, pairs)
                    target[*spot] = (pairs * cross - left * right) * lax.rsqrt(var_left * var_right)
            if mirror is not None:
                mirror[...] = target[...].T

        def tile_at(kind, index):
            index = jnp.int32(index)
            if kind == "own":
                return index, index
            if kind == "plain":
                return lax.rem(index, assets // TILE), lax.div(index, assets // TILE)
            column = jnp.int32(1)
            for j in range(2, assets // TILE):
                column = column + (index >= j * (j - 1) // 2).astype(jnp.int32)
            return index - lax.div(column * (column - 1), 2), column

        def run(steps, turns, kind, buf, sem, mirror_buf, mirror_sem):
            def tiles(step):
                return [tile_at(kind, step * turns + u) for u in range(turns)]

            def copies(step):
                slot = lax.rem(step, 2)
                for u, (i, j) in enumerate(tiles(step)):
                    yield pltpu.make_async_copy(buf.at[slot, u], out.at[tile(i), tile(j)], sem.at[slot, u])
                    if mirror_buf is not None:
                        yield pltpu.make_async_copy(mirror_buf.at[slot, u], out.at[tile(j), tile(i)], mirror_sem.at[slot, u])

            def waits(step):
                for copy in copies(step):
                    copy.wait()

            def one(step, carry):
                slot = lax.rem(step, 2)

                @pl.when(step >= 2)
                def _():
                    waits(step - 2)

                at = tiles(step)

                def finish(u):
                    i, j = at[u]
                    combine(i, j + shift, u % 2, buf.at[slot, u], None if mirror_buf is None else mirror_buf.at[slot, u])

                shift = 0 if plan.whole else first
                for u, (i, j) in enumerate(at):
                    if kind == "own":
                        own_products(i, u)
                    else:
                        products(i, j + shift, u)
                    if u:
                        finish(u - 1)
                finish(turns - 1)
                for copy in copies(step):
                    copy.start()
                return carry

            lax.fori_loop(0, steps, one, 0)
            return lambda: [waits(step) for step in range(max(steps - 2, 0), steps)]

        def run_lagged(steps, turns, kind):
            final = steps * turns - 1

            def tiles(step):
                lagging = jnp.where(step == 0, final, step * turns - 1)
                return [tile_at(kind, lagging)] + [tile_at(kind, step * turns + u) for u in range(turns)]

            def pair(i, j, source, mirror, sem, mirror_sem):
                yield pltpu.make_async_copy(source, out.at[tile(i), tile(j)], sem)
                yield pltpu.make_async_copy(mirror, out.at[tile(j), tile(i)], mirror_sem)

            def copies(step):
                slot = lax.rem(step, 2)
                for u, (i, j) in enumerate(tiles(step)[:turns]):
                    yield from pair(i, j, buf_m.at[slot, u], buf_t.at[slot, u], sem_m.at[slot, u], sem_t.at[slot, u])

            def waits(step):
                for copy in copies(step):
                    copy.wait()

            def one(step, carry):
                slot = lax.rem(step, 2)

                @pl.when(step >= 2)
                def _():
                    waits(step - 2)

                at = tiles(step)
                for u in range(turns):
                    products(*at[u + 1], u, last=u == turns - 1)
                    combine(*at[u], slot_of(u - 1, u == 0), buf_m.at[slot, u], buf_t.at[slot, u])
                for copy in copies(step):
                    copy.start()
                return carry

            lax.fori_loop(0, steps, one, 0)
            i, j = tile_at(kind, final)
            combine(i, j, 2, buf_e.at[0], buf_e.at[1])
            rest = list(pair(i, j, buf_e.at[0], buf_e.at[1], sem_e.at[0], sem_e.at[1]))
            for copy in rest:
                copy.start()

            def end():
                for step in range(max(steps - 2, 0), steps):
                    waits(step)
                for copy in rest:
                    copy.wait()

            return end

        ends = []
        if plan.whole:
            if plan.mirrored[0] > 2:
                ends.append(run_lagged(*plan.mirrored, "mirror"))
            else:
                ends.append(run(*plan.mirrored, "mirror", buf_m, sem_m, buf_t, sem_t))
            ends.append(run(*plan.plain, "own", buf_p, sem_p, None, None))
        else:
            ends.append(run(*plan.plain, "plain", buf_p, sem_p, None, None))
        for end in ends:
            end()

    pl.run_scoped(body, *([pltpu.ACC(0)((TILE, TILE), f32)] * 4 + [pltpu.ACC(1)((TILE, TILE), f32)] * 4))


def turns_of(count, most):
    turns = max(t for t in range(1, most + 1) if count % t == 0)
    return count // turns, turns


def correlation(pieces, begins, ends, height, width, members, whole):
    assets = begins.shape[1]
    every = assets // TILE
    own = width // TILE
    mirrored = every * (every - 1) // 2 if whole else 0
    plain = every if whole else every * own
    plan = Plan(
        pieces=len(pieces),
        height=height,
        width=width,
        members=members,
        whole=whole,
        mirrored=turns_of(mirrored, UNROLL) if mirrored else (0, 1),
        plain=turns_of(plain, UNROLL_OWN),
    )
    turns_m, turns_p = plan.mirrored[1], plan.plain[1]
    f32, bf16 = jnp.float32, jnp.bfloat16
    vmem = pl.BlockSpec(memory_space=pltpu.VMEM)
    depth = len(pieces) * height
    flops = 2 * depth * TILE * TILE * (11 * mirrored + (7 if whole else 11) * plain)
    return pl.pallas_call(
        functools.partial(correlation_kernel, plan),
        out_shape=jax.ShapeDtypeStruct((assets, width), f32),
        in_specs=[vmem] * (len(pieces) + 2),
        out_specs=pl.BlockSpec(memory_space=pl.ANY),
        scratch_shapes=[pltpu.VMEM((assets, depth), bf16)] * 5
        + [pltpu.VMEM((assets, LANES), f32)] * 2
        + [
            pltpu.VMEM((3, 5, TILE, TILE), f32),
            pltpu.VMEM((2, turns_m, TILE, TILE), f32),
            pltpu.VMEM((2, turns_m, TILE, TILE), f32),
            pltpu.VMEM((2, turns_p, TILE, TILE), f32),
            pltpu.VMEM((2, TILE, TILE), f32),
            pltpu.SemaphoreType.DMA((2, turns_m)),
            pltpu.SemaphoreType.DMA((2, turns_m)),
            pltpu.SemaphoreType.DMA((2, turns_p)),
            pltpu.SemaphoreType.DMA((2,)),
        ],
        cost_estimate=pl.CostEstimate(flops=flops, bytes_accessed=4 * assets * width, transcendentals=assets * width),
        compiler_params=pltpu.CompilerParams(vmem_limit_bytes=32 * 2**20),
        name="correlation",
    )(*pieces, begins, ends)


def on_device(returns, windows, listed_from, listed_until):
    height, width = returns.shape
    members = SPAN // height // 2
    rows = lax.all_gather(returns, "asset", axis=1, tiled=True)
    after = (lax.axis_index("tm") + 1) * height
    earliest = jnp.maximum(after - windows[0], 0)
    begins = jnp.maximum(listed_from, earliest).astype(jnp.float32)[None]
    ends = jnp.minimum(listed_until, after).astype(jnp.float32)[None]
    pieces, (begins, ends) = gather_span(rows, "tm", members, (begins, ends))
    whole = lax.axis_size("asset") == 1
    return correlation(pieces, begins, ends, height, width, members, whole)[None]


def solution(mesh):
    placed = (P("tm", "asset"), P("tm"), P(), P())
    step = jax.shard_map(on_device, mesh=mesh, in_specs=placed, out_specs=P("tm", None, "asset"), check_vma=False)

    def call(*args):
        with jax.sharding.use_abstract_mesh(mesh.abstract_mesh):
            return step(*args)

    return call
```

```python
import dataclasses
import functools

import jax
import jax.numpy as jnp
from jax import lax
from jax.experimental import pallas as pl
from jax.experimental.pallas import tpu as pltpu
from jax.sharding import PartitionSpec as P

SPAN = 256
TILE = 256
LANES = 128
UNROLL = 4
UNROLL_OWN = 8


@dataclasses.dataclass(frozen=True)
class Plan:
    pieces: int
    height: int
    width: int
    members: int
    whole: bool
    mirrored: tuple
    plain: tuple


def cycle(array, axis, by):
    devices = lax.axis_size(axis)
    return lax.ppermute(array, axis, [(i, (i + by) % devices) for i in range(devices)])


def swap(array, axis, by):
    devices = lax.axis_size(axis)
    return lax.ppermute(array, axis, [(i, i ^ by) for i in range(devices)])


def gather_span(rows, axis, members, early):
    member = lax.rem(lax.axis_index(axis), members)
    own = jnp.where(member >= 0, rows, 0.0)
    before, own, *early = lax.optimization_barrier((cycle(rows, axis, members), own, *early))
    middle = [swap(before, axis, by) for by in range(2, members, 2)]
    before2 = cycle(rows, axis, 2 * members)

    def outer(by):
        return jnp.where((member ^ by) >= member, own, before2)

    ends = [swap(outer(by), axis, by) for by in range(2, members, 2)]
    relayed = [swap(piece, axis, 1) for piece in (before, *middle, outer(1), *ends)]
    return [before, *middle, *relayed[: members // 2], own, *ends, *relayed[members // 2 :]], early


def correlation_kernel(plan, *refs):
    pieces = refs[: plan.pieces]
    begins, ends_at, out = refs[plan.pieces : plan.pieces + 3]
    (hi, lo, sq, sl, on, low, high, sums, buf_m, buf_t, buf_p, buf_e, sem_m, sem_t, sem_p, sem_e) = refs[plan.pieces + 3 :]
    assets = begins.shape[1]
    f32, bf16 = jnp.float32, jnp.bfloat16
    depth = plan.height * plan.pieces

    position = lax.axis_index("tm")
    member = lax.rem(position, plan.members)
    group = lax.div(position, plan.members)
    first = lax.axis_index("asset") * (plan.width // TILE)

    def block_start(piece):
        order = [0] + list(range(2, plan.members, 2)) + [1] + [by ^ 1 for by in range(2, plan.members, 2)]
        other = member ^ order[piece % plan.members]
        if piece < plan.members:
            source = group - 1
        else:
            source = jnp.where(other > member, group - 2, group)
        return (source * plan.members + other) * plan.height

    lane = lax.broadcasted_iota(jnp.int32, (8, depth), 1)
    days = lax.rem(lane, plan.height)
    for piece in range(plan.pieces):
        days = days + jnp.where(lax.div(lane, plan.height) == piece, block_start(piece), 0)
    days = days.astype(f32)[:1]

    def split(x):
        high_part = x.astype(bf16)
        return high_part, (x - high_part.astype(f32)).astype(bf16)

    def prepare(step, carry):
        cols = pl.ds(pl.multiple_of(step * TILE, TILE), TILE)
        begin = jnp.broadcast_to(begins[:, cols], (LANES, TILE)).T
        end = jnp.broadcast_to(ends_at[:, cols], (LANES, TILE)).T
        low[cols, :] = begin
        high[cols, :] = end
        for part in range(0, depth, LANES):
            days_at = days[:, part : part + LANES]
            at = pl.ds(part, LANES)
            count = LANES // plan.height
            which = range(part // plan.height, part // plan.height + count)
            value = jnp.concatenate([pieces[p][:, cols] for p in which], axis=0).T
            live = (days_at >= begin) & (days_at < end)
            value = jnp.where(live, value, 0.0)
            on[cols, at] = jnp.where(live, 1.0, 0.0).astype(bf16)
            hi[cols, at], lo[cols, at] = split(value)
            sq[cols, at], sl[cols, at] = split(value * value)
        return carry

    lax.fori_loop(0, assets // TILE, prepare, 0)

    def body(*accs):
        units = accs[:4], accs[4:]
        for acc in accs:
            sums[0, 0] = pltpu.matmul_pop(acc)
        push_at = [0, 0]
        acc_at = [0, 0]

        def tile(index):
            return pl.ds(pl.multiple_of(index * TILE, TILE), TILE)

        def load(ref, j, unit):
            pltpu.matmul_push_rhs(ref[tile(j), :], staging_register=push_at[unit] % 2, mxu_index=unit, transpose=True)
            push_at[unit] += 1
            return (push_at[unit] - 1) % 2

        def fresh(unit):
            acc_at[unit] += 1
            return units[unit][(acc_at[unit] - 1) % 4]

        def add(acc, ref, i, register=None):
            pltpu.matmul_acc_lhs(acc, ref[tile(i), :], load_staged_rhs=register)

        def slot_of(turn, last):
            return 2 if last else turn % 2

        def products(i, j, turn, last=False):
            x, y = turn % 2, 1 - turn % 2
            left, left_sq, right_sq = fresh(x), fresh(x), fresh(x)
            cross, right = fresh(y), fresh(y)
            r = load(on, j, x)
            s = load(hi, j, y)
            add(left, hi, i, r)
            add(cross, hi, i, s)
            r = load(sq, j, x)
            s = load(lo, j, y)
            add(left, lo, i)
            add(cross, lo, i)
            add(left_sq, sq, i)
            add(right, on, i)
            add(left_sq, sl, i)
            add(cross, hi, i, s)
            add(right_sq, on, i, r)
            r = load(sl, j, x)
            add(right, on, i)
            add(right_sq, on, i, r)
            for k, acc in enumerate((left, cross, left_sq, right, right_sq)):
                sums[slot_of(turn, last), k] = pltpu.matmul_pop(acc)

        def own_products(i, turn):
            x, y = turn % 2, 1 - turn % 2
            left, left_sq = fresh(x), fresh(x)
            cross = fresh(y)
            r = load(on, i, x)
            s = load(hi, i, y)
            add(left, hi, i, r)
            add(cross, hi, i, s)
            s = load(lo, i, y)
            add(left, lo, i)
            add(cross, lo, i)
            add(left_sq, sq, i)
            add(cross, hi, i, s)
            add(left_sq, sl, i)
            for k, acc in enumerate((left, cross, left_sq)):
                sums[turn % 2, k] = pltpu.matmul_pop(acc)
            sums[turn % 2, 3] = sums[turn % 2, 0].T
            sums[turn % 2, 4] = sums[turn % 2, 2].T

        def combine(i, j, at, target, mirror):
            step = 16
            for row in range(0, TILE, step):
                mine = pl.ds(pl.multiple_of(i * TILE + row, step), step)
                for col in range(0, TILE, LANES):
                    spot = (pl.ds(row, step), pl.ds(col, LANES))
                    theirs = pl.ds(pl.multiple_of(j * TILE + col, LANES), LANES)
                    begin, end = begins[:, theirs], ends_at[:, theirs]
                    pairs = jnp.maximum(jnp.minimum(high[mine, :], end) - jnp.maximum(low[mine, :], begin), 1.0)
                    left, cross, left_sq, right, right_sq = (sums[at, k, *spot] for k in range(5))
                    var_left = jnp.maximum(pairs * left_sq - left * left, pairs)
                    var_right = jnp.maximum(pairs * right_sq - right * right, pairs)
                    target[*spot] = (pairs * cross - left * right) * lax.rsqrt(var_left * var_right)
            if mirror is not None:
                mirror[...] = target[...].T

        def tile_at(kind, index):
            index = jnp.int32(index)
            if kind == "own":
                return index, index
            if kind == "plain":
                return lax.rem(index, assets // TILE), lax.div(index, assets // TILE)
            column = jnp.int32(1)
            for j in range(2, assets // TILE):
                column = column + (index >= j * (j - 1) // 2).astype(jnp.int32)
            return index - lax.div(column * (column - 1), 2), column

        def run(steps, turns, kind, buf, sem, mirror_buf, mirror_sem):
            def tiles(step):
                return [tile_at(kind, step * turns + u) for u in range(turns)]

            def copies(step):
                slot = lax.rem(step, 2)
                for u, (i, j) in enumerate(tiles(step)):
                    yield pltpu.make_async_copy(buf.at[slot, u], out.at[tile(i), tile(j)], sem.at[slot, u])
                    if mirror_buf is not None:
                        yield pltpu.make_async_copy(mirror_buf.at[slot, u], out.at[tile(j), tile(i)], mirror_sem.at[slot, u])

            def waits(step):
                for copy in copies(step):
                    copy.wait()

            def one(step, carry):
                slot = lax.rem(step, 2)

                @pl.when(step >= 2)
                def _():
                    waits(step - 2)

                at = tiles(step)

                def finish(u):
                    i, j = at[u]
                    combine(i, j + shift, u % 2, buf.at[slot, u], None if mirror_buf is None else mirror_buf.at[slot, u])

                shift = 0 if plan.whole else first
                for u, (i, j) in enumerate(at):
                    if kind == "own":
                        own_products(i, u)
                    else:
                        products(i, j + shift, u)
                    if u:
                        finish(u - 1)
                finish(turns - 1)
                for copy in copies(step):
                    copy.start()
                return carry

            lax.fori_loop(0, steps, one, 0)
            return lambda: [waits(step) for step in range(max(steps - 2, 0), steps)]

        def run_lagged(steps, turns, kind):
            final = steps * turns - 1

            def tiles(step):
                lagging = jnp.where(step == 0, final, step * turns - 1)
                return [tile_at(kind, lagging)] + [tile_at(kind, step * turns + u) for u in range(turns)]

            def pair(i, j, source, mirror, sem, mirror_sem):
                yield pltpu.make_async_copy(source, out.at[tile(i), tile(j)], sem)
                yield pltpu.make_async_copy(mirror, out.at[tile(j), tile(i)], mirror_sem)

            def copies(step):
                slot = lax.rem(step, 2)
                for u, (i, j) in enumerate(tiles(step)[:turns]):
                    yield from pair(i, j, buf_m.at[slot, u], buf_t.at[slot, u], sem_m.at[slot, u], sem_t.at[slot, u])

            def waits(step):
                for copy in copies(step):
                    copy.wait()

            def one(step, carry):
                slot = lax.rem(step, 2)

                @pl.when(step >= 2)
                def _():
                    waits(step - 2)

                at = tiles(step)
                for u in range(turns):
                    products(*at[u + 1], u, last=u == turns - 1)
                    combine(*at[u], slot_of(u - 1, u == 0), buf_m.at[slot, u], buf_t.at[slot, u])
                for copy in copies(step):
                    copy.start()
                return carry

            lax.fori_loop(0, steps, one, 0)
            i, j = tile_at(kind, final)
            combine(i, j, 2, buf_e.at[0], buf_e.at[1])
            rest = list(pair(i, j, buf_e.at[0], buf_e.at[1], sem_e.at[0], sem_e.at[1]))
            for copy in rest:
                copy.start()

            def end():
                for step in range(max(steps - 2, 0), steps):
                    waits(step)
                for copy in rest:
                    copy.wait()

            return end

        ends = []
        if plan.whole:
            if plan.mirrored[0] > 2:
                ends.append(run_lagged(*plan.mirrored, "mirror"))
            else:
                ends.append(run(*plan.mirrored, "mirror", buf_m, sem_m, buf_t, sem_t))
            ends.append(run(*plan.plain, "own", buf_p, sem_p, None, None))
        else:
            ends.append(run(*plan.plain, "plain", buf_p, sem_p, None, None))
        for end in ends:
            end()

    pl.run_scoped(body, *([pltpu.ACC(0)((TILE, TILE), f32)] * 4 + [pltpu.ACC(1)((TILE, TILE), f32)] * 4))


def turns_of(count, most):
    turns = max(t for t in range(1, most + 1) if count % t == 0)
    return count // turns, turns


def correlation(pieces, begins, ends, height, width, members, whole):
    assets = begins.shape[1]
    every = assets // TILE
    own = width // TILE
    mirrored = every * (every - 1) // 2 if whole else 0
    plain = every if whole else every * own
    plan = Plan(
        pieces=len(pieces),
        height=height,
        width=width,
        members=members,
        whole=whole,
        mirrored=turns_of(mirrored, UNROLL) if mirrored else (0, 1),
        plain=turns_of(plain, UNROLL_OWN),
    )
    turns_m, turns_p = plan.mirrored[1], plan.plain[1]
    f32, bf16 = jnp.float32, jnp.bfloat16
    vmem = pl.BlockSpec(memory_space=pltpu.VMEM)
    depth = len(pieces) * height
    flops = 2 * depth * TILE * TILE * (11 * mirrored + (7 if whole else 11) * plain)
    return pl.pallas_call(
        functools.partial(correlation_kernel, plan),
        out_shape=jax.ShapeDtypeStruct((assets, width), f32),
        in_specs=[vmem] * (len(pieces) + 2),
        out_specs=pl.BlockSpec(memory_space=pl.ANY),
        scratch_shapes=[pltpu.VMEM((assets, depth), bf16)] * 5
        + [pltpu.VMEM((assets, LANES), f32)] * 2
        + [
            pltpu.VMEM((3, 5, TILE, TILE), f32),
            pltpu.VMEM((2, turns_m, TILE, TILE), f32),
            pltpu.VMEM((2, turns_m, TILE, TILE), f32),
            pltpu.VMEM((2, turns_p, TILE, TILE), f32),
            pltpu.VMEM((2, TILE, TILE), f32),
            pltpu.SemaphoreType.DMA((2, turns_m)),
            pltpu.SemaphoreType.DMA((2, turns_m)),
            pltpu.SemaphoreType.DMA((2, turns_p)),
            pltpu.SemaphoreType.DMA((2,)),
        ],
        cost_estimate=pl.CostEstimate(flops=flops, bytes_accessed=4 * assets * width, transcendentals=assets * width),
        compiler_params=pltpu.CompilerParams(vmem_limit_bytes=32 * 2**20),
        name="correlation",
    )(*pieces, begins, ends)


def on_device(returns, windows, listed_from, listed_until):
    height, width = returns.shape
    members = SPAN // height // 2
    rows = lax.all_gather(returns, "asset", axis=1, tiled=True)
    after = (lax.axis_index("tm") + 1) * height
    earliest = jnp.maximum(after - windows[0], 0)
    begins = jnp.maximum(listed_from, earliest).astype(jnp.float32)[None]
    ends = jnp.minimum(listed_until, after).astype(jnp.float32)[None]
    pieces, (begins, ends) = gather_span(rows, "tm", members, (begins, ends))
    whole = lax.axis_size("asset") == 1
    return correlation(pieces, begins, ends, height, width, members, whole)[None]


def solution(mesh):
    placed = (P("tm", "asset"), P("tm"), P(), P())
    step = jax.shard_map(on_device, mesh=mesh, in_specs=placed, out_specs=P("tm", None, "asset"), check_vma=False)

    def call(*args):
        with jax.sharding.use_abstract_mesh(mesh.abstract_mesh):
            return step(*args)

    return call
```
